8 devices in a mesh: fsdp: 2 (over z, y), ep: 4 (over x, core).
Axes of the slice: x: 2, y: 2, z: 1, core: 2. Of those that a mesh axis runs over, the one named last changes fastest.
Arguments:
- x_in: bfloat16 [2, 16384, 896], P(None, ('fsdp', 'ep'))
- dy_out: bfloat16 [2, 16384, 896], P(None, ('fsdp', 'ep'))
- expert_idx: int32 [2, 16384, 8], P(None, ('fsdp', 'ep'))
- gate_prob: float32 [2, 16384, 8], P(None, ('fsdp', 'ep'))
- w_one: bfloat16 [256, 896, 256], P('ep', 'fsdp')
- w_two: bfloat16 [256, 256, 896], P('ep', None, 'fsdp')
- w_three: bfloat16 [256, 896, 256], P('ep', 'fsdp')
Outputs:
- output 1: bfloat16 [2, 16384, 896], P(None, ('fsdp', 'ep'))
- output 2: float32 [2, 16384, 8], P(None, ('fsdp', 'ep'))
- output 3: float32 [256, 896, 256], P('ep', 'fsdp')
- output 4: float32 [256, 256, 896], P('ep', None, 'fsdp')
- output 5: float32 [256, 896, 256], P('ep', 'fsdp')
All inputs are finite; a program needn't handle non-finite values.
Results may differ from the reference program's by a relative error of at most 0.001.
Values are sent between devices in bfloat16 or wider.
A program may use at most 1 GiB of HBM per device.

```python
import jax
import jax.numpy as jnp
from jax import lax

D_MODEL = 896
FF_DIM = 256
EXPERTS = 256
TOP_K = 8
TOK_DEV = 2048
SOURCES = 8
MICRO_BATCHES = 2
CAPACITY = 80

TOKENS = SOURCES * TOK_DEV
N_CHOICE = TOK_DEV * TOP_K


def draw_routing(key):
    key_hot, key_bias, key_score = jax.random.split(key, 3)
    expert_ids = jnp.arange(EXPERTS, dtype=jnp.int32)
    hot_ids = jax.random.randint(key_hot, (MICRO_BATCHES, SOURCES, 1, 1), 0, EXPERTS)
    forced = jnp.arange(TOK_DEV)[:, None] < CAPACITY
    hot_bonus = jnp.where(expert_ids == hot_ids, 1, 0) * jnp.where(forced, 4096, 512)
    source_bias = jax.random.randint(key_bias, (MICRO_BATCHES, SOURCES, 1, EXPERTS), 0, 512)
    rand_score = jax.random.randint(key_score, (MICRO_BATCHES, SOURCES, TOK_DEV, EXPERTS), 0, 1024)
    total_score = (rand_score + source_bias + hot_bonus) * EXPERTS + expert_ids
    chosen = lax.top_k(total_score, TOP_K)[1]
    return chosen.reshape(MICRO_BATCHES, TOKENS, TOP_K).astype(jnp.int32)


def setup_inputs(seed: int = 0) -> dict:
    key_list = jax.random.split(jax.random.key(seed), 7)
    x_vals = jax.random.normal(key_list[0], (MICRO_BATCHES, TOKENS, D_MODEL), jnp.float32)
    dy_vals = jax.random.normal(key_list[1], (MICRO_BATCHES, TOKENS, D_MODEL), jnp.float32)
    routing = draw_routing(key_list[2])
    gate_vals = jax.random.uniform(key_list[3], (MICRO_BATCHES, TOKENS, TOP_K), jnp.float32, 0.2, 1.0)
    w_one = jax.random.normal(key_list[4], (EXPERTS, D_MODEL, FF_DIM), jnp.float32) * D_MODEL ** -0.5
    w_two = jax.random.normal(key_list[5], (EXPERTS, FF_DIM, D_MODEL), jnp.float32) * FF_DIM ** -0.5
    w_three = jax.random.normal(key_list[6], (EXPERTS, D_MODEL, FF_DIM), jnp.float32) * D_MODEL ** -0.5
    return {'x_in': x_vals.astype(jnp.bfloat16), 'dy_out': dy_vals.astype(jnp.bfloat16), 'expert_idx': routing, 'gate_prob': gate_vals, 'w_one': w_one.astype(jnp.bfloat16), 'w_two': w_two.astype(jnp.bfloat16), 'w_three': w_three.astype(jnp.bfloat16)}


def slot_holder(ids_flat):
    one_hot = (ids_flat[:, None] == jnp.arange(EXPERTS, dtype=jnp.int32)[None, :]).astype(jnp.int32)
    position = jnp.sum((jnp.cumsum(one_hot, axis=0) - one_hot) * one_hot, axis=1)
    choice_slot = jnp.where(position < CAPACITY, ids_flat * CAPACITY + position, EXPERTS * CAPACITY)
    holder = jnp.full((EXPERTS * CAPACITY + 1,), N_CHOICE, jnp.int32)
    holder = holder.at[choice_slot].set(jnp.arange(N_CHOICE, dtype=jnp.int32))
    return holder[:EXPERTS * CAPACITY]


def expert_rows(x_rows, dy_rows, gate_rows, w_a, w_b, w_c):
    h_one = jnp.dot(x_rows, w_a, preferred_element_type=jnp.float32)
    h_three = jnp.dot(x_rows, w_c, preferred_element_type=jnp.float32)
    sigma_one = jax.nn.sigmoid(h_one)
    silu_one = h_one * sigma_one
    act_bf = (silu_one * h_three).astype(jnp.bfloat16)
    y_rows = jnp.dot(act_bf, w_b, preferred_element_type=jnp.float32)
    dg_rows = jnp.sum(dy_rows.astype(jnp.float32) * y_rows, axis=1)
    g_rows = (gate_rows[:, None] * dy_rows.astype(jnp.float32)).astype(jnp.bfloat16)
    d_act = jnp.dot(g_rows, w_b.T, preferred_element_type=jnp.float32)
    dh_three = (d_act * silu_one).astype(jnp.bfloat16)
    dh_one = (d_act * h_three * sigma_one * (1.0 + h_one * (1.0 - sigma_one))).astype(jnp.bfloat16)
    dx_rows = (jnp.dot(dh_one, w_a.T, preferred_element_type=jnp.float32) + jnp.dot(dh_three, w_c.T, preferred_element_type=jnp.float32)).astype(jnp.bfloat16)
    gw_one = jnp.dot(x_rows.T, dh_one, preferred_element_type=jnp.float32)
    gw_two = jnp.dot(act_bf.T, g_rows, preferred_element_type=jnp.float32)
    gw_three = jnp.dot(x_rows.T, dh_three, preferred_element_type=jnp.float32)
    return dx_rows, dg_rows, gw_one, gw_two, gw_three


def reference(x_in, dy_out, expert_idx, gate_prob, w_one, w_two, w_three):
    total_choices = MICRO_BATCHES * TOKENS * TOP_K
    holder = lax.map(slot_holder, expert_idx.reshape(MICRO_BATCHES * SOURCES, N_CHOICE))
    block_base = jnp.arange(MICRO_BATCHES * SOURCES, dtype=jnp.int32)[:, None] * N_CHOICE
    slot_choice = jnp.where(holder < N_CHOICE, holder + block_base, total_choices)
    slot_choice = jnp.transpose(slot_choice.reshape(MICRO_BATCHES, SOURCES, EXPERTS, CAPACITY), (2, 0, 1, 3))
    slot_choice = slot_choice.reshape(EXPERTS, MICRO_BATCHES, SOURCES * CAPACITY)
    zero_row = jnp.zeros((1, D_MODEL), x_in.dtype)
    x_flat = jnp.concatenate([x_in.reshape(MICRO_BATCHES * TOKENS, D_MODEL), zero_row], axis=0)
    dy_flat = jnp.concatenate([dy_out.reshape(MICRO_BATCHES * TOKENS, D_MODEL), zero_row], axis=0)
    gate_flat = jnp.concatenate([gate_prob.reshape(total_choices), jnp.zeros((1,), gate_prob.dtype)])

    def expert_step(scan_state, per_expert):
        dx_acc, dg_acc = scan_state
        w_a, w_b, w_c, choices = per_expert
        grad_one = jnp.zeros((D_MODEL, FF_DIM), jnp.float32)
        grad_two = jnp.zeros((FF_DIM, D_MODEL), jnp.float32)
        grad_three = jnp.zeros((D_MODEL, FF_DIM), jnp.float32)
        for mb_index in range(MICRO_BATCHES):
            pick_ids = choices[mb_index]
            tok_ids = pick_ids // TOP_K
            dx_rows, dg_rows, gw_one, gw_two, gw_three = expert_rows(x_flat[tok_ids], dy_flat[tok_ids], gate_flat[pick_ids], w_a, w_b, w_c)
            dx_acc = dx_acc.at[tok_ids].add(dx_rows.astype(jnp.float32))
            dg_acc = dg_acc.at[pick_ids].set(dg_rows)
            grad_one = grad_one + gw_one
            grad_two = grad_two + gw_two
            grad_three = grad_three + gw_three
        return (dx_acc, dg_acc), (grad_one, grad_two, grad_three)

    start_state = (jnp.zeros((MICRO_BATCHES * TOKENS + 1, D_MODEL), jnp.float32), jnp.zeros((total_choices + 1,), jnp.float32))
    end_state, grad_stack = lax.scan(expert_step, start_state, (w_one, w_two, w_three, slot_choice))
    dx_in = end_state[0][:MICRO_BATCHES * TOKENS].astype(jnp.bfloat16).reshape(MICRO_BATCHES, TOKENS, D_MODEL)
    d_gate = end_state[1][:total_choices].reshape(MICRO_BATCHES, TOKENS, TOP_K)
    return (dx_in, d_gate, grad_stack[0], grad_stack[1], grad_stack[2])
```

```python
import functools

import jax
import jax.numpy as jnp
from jax import lax
from jax.experimental import pallas as pl
from jax.experimental.pallas import tpu as pltpu
from jax.sharding import PartitionSpec as P


BF = jnp.bfloat16
F32 = jnp.float32
NT = (((1,), (1,)), ((), ()))
TN = (((0,), (0,)), ((), ()))
LANES = 128
GROUP = 8
CHUNKS = (16, 16, 16, 8, 8)
VMEM_LIMIT = 62 * 2**20


def capacity_of(tok_rows, top_k, experts):
    return 8 * ((5 * tok_rows * top_k + 32 * experts - 1) // (32 * experts))


def params():
    return pltpu.CompilerParams(vmem_limit_bytes=VMEM_LIMIT)


def cost(flops, nbytes):
    return pl.CostEstimate(flops=int(flops), bytes_accessed=int(nbytes), transcendentals=0)


def route_kernel(base_ref, info_ref, pos_ref, gate_ref, choice_ref, *, top_k, capacity):
    experts, tokens = pos_ref.shape[1:]
    ids = (lax.broadcasted_iota(jnp.int32, (experts, tokens), 0) + base_ref[0]).astype(F32)
    member = jnp.zeros((experts, tokens), F32)
    gate = jnp.zeros((experts, tokens), F32)
    choice = jnp.zeros((experts, tokens), F32)
    for j in range(top_k):
        hit = ids == info_ref[0, j:j + 1, :]
        member = jnp.where(hit, 1.0, member)
        gate = jnp.where(hit, info_ref[0, top_k + j:top_k + j + 1, :], gate)
        choice = jnp.where(hit, float(j), choice)
    gate_ref[0] = gate
    choice_ref[0] = choice
    step = 256
    earlier = (lax.broadcasted_iota(jnp.int32, (step, step), 0) < lax.broadcasted_iota(jnp.int32, (step, step), 1))
    earlier = jnp.where(earlier, 1.0, 0.0).astype(BF)
    carry = jnp.zeros((experts, 1), F32)
    for t in range(0, tokens, step):
        block = member[:, t:t + step]
        position = carry + jnp.dot(block.astype(BF), earlier, preferred_element_type=F32)
        kept = jnp.logical_and(block > 0.5, position < capacity)
        pos_ref[0, :, t:t + step] = jnp.where(kept, position, -1.0).astype(BF)
        carry = carry + jnp.sum(block, axis=1, keepdims=True)


def route(base, info, experts, top_k, capacity):
    units, rows, tokens = info.shape
    out = pl.BlockSpec((1, experts, tokens), lambda u: (u, 0, 0))
    shape = (units, experts, tokens)
    return pl.pallas_call(
        functools.partial(route_kernel, top_k=top_k, capacity=capacity),
        grid=(units,),
        in_specs=[pl.BlockSpec(memory_space=pltpu.SMEM), pl.BlockSpec((1, rows, tokens), lambda u: (u, 0, 0))],
        out_specs=[out, out, out],
        out_shape=[jax.ShapeDtypeStruct(shape, BF), jax.ShapeDtypeStruct(shape, F32), jax.ShapeDtypeStruct(shape, F32)],
        compiler_params=params(),
        cost_estimate=cost(units * 1e9, units * experts * tokens * 10),
        name="route",
    )(base, info)


def gather_kernel(*refs, units, aliased):
    pos_ref, gate_ref, choice_ref = refs[:3]
    blocks = refs[3:3 + units]
    refs = refs[3 + units + (2 if aliased else 0):]
    rows_ref, meta_ref, held, sems = refs
    group, _, capacity, width = rows_ref.shape
    tokens = pos_ref.shape[2]
    u, g = pl.program_id(0), pl.program_id(1)

    def fetch(i):
        return pltpu.make_async_copy(blocks[i], held.at[i % 2], sems.at[i % 2])

    for i in range(units):
        @pl.when(jnp.logical_and(u == i, g == 0))
        def _(i=i):
            if i == 0:
                fetch(0).start()
            if i + 1 < units:
                fetch(i + 1).start()
            fetch(i).wait()

    slot = lax.broadcasted_iota(jnp.int32, (capacity, tokens), 0).astype(F32)
    slot_bf = slot.astype(BF)
    lane = lax.broadcasted_iota(jnp.int32, (capacity, LANES), 1)
    picks = []
    for e in range(group):
        row = pos_ref[0, e:e + 1, :]
        picks.append(jnp.where(jnp.broadcast_to(row, (capacity, tokens)) == slot_bf, jnp.ones((), BF), jnp.zeros((), BF)))
        hit = jnp.broadcast_to(row.astype(F32), (capacity, tokens)) == slot
        gate = jnp.sum(jnp.where(hit, gate_ref[0, e:e + 1, :], 0.0), axis=1, keepdims=True)
        choice = jnp.sum(jnp.where(hit, choice_ref[0, e:e + 1, :], 0.0), axis=1, keepdims=True)
        meta_ref[e, 0] = jnp.where(lane == 0, gate, choice)
    one_hot = jnp.concatenate(picks, axis=0)
    rows = jnp.dot(one_hot, held[u % 2], preferred_element_type=F32).astype(BF)
    rows_ref[...] = rows.reshape(group, 1, capacity, width)


def gather(tables, start, blocks, place, total, capacity, buffers):
    pos, gate, choice = tables
    experts, tokens = pos.shape[1:]
    width = blocks[0].shape[1]
    first, stride = place
    units = len(blocks)
    offset, skip = start
    table = pl.BlockSpec((1, GROUP, tokens), lambda u, g: (offset + skip * u, g, 0))
    anywhere = pl.BlockSpec(memory_space=pl.ANY)
    out_map = lambda u, g: (g, first + stride * u, 0, 0)
    aliased = buffers is not None
    n_in = 3 + units
    return pl.pallas_call(
        functools.partial(gather_kernel, units=units, aliased=aliased),
        grid=(units, experts // GROUP),
        in_specs=[table] * 3 + [anywhere] * (units + (2 if aliased else 0)),
        out_specs=[pl.BlockSpec((GROUP, 1, capacity, width), out_map), pl.BlockSpec((GROUP, 1, capacity, LANES), out_map)],
        out_shape=[
            jax.ShapeDtypeStruct((experts, total, capacity, width), BF),
            jax.ShapeDtypeStruct((experts, total, capacity, LANES), F32),
        ],
        scratch_shapes=[pltpu.VMEM((2, tokens, width), BF), pltpu.SemaphoreType.DMA((2,))],
        input_output_aliases={n_in: 0, n_in + 1: 1} if aliased else {},
        compiler_params=params(),
        cost_estimate=cost(2 * units * experts * capacity * tokens * width, units * experts * capacity * width * 4),
        name="gather",
    )(pos, gate, choice, *blocks, *(buffers if aliased else ()))


def expert_kernel(*refs, aliased, own, mine):
    (half_ref, rows_ref, meta_ref, w1, w3, w2, w_got) = refs[:7]
    refs = refs[7 + (3 if aliased else 0):]
    (dw1, dw3, dw2, dx_mine, dx_peer, dg_mine, dg_peer, w_all, g_s, a_s, dh_s, acc_s) = refs
    _, units, capacity, width = rows_ref.shape
    d = width // 2
    half, ff = w1.shape[1:]
    total = units * capacity
    f = half_ref[0]
    near = pl.ds(pl.multiple_of(f * half, half), half)
    far = pl.ds(pl.multiple_of((1 - f) * half, half), half)
    w_all[far, :] = w_got[0]
    w_all[near, 0:ff] = w1[0]
    w_all[near, ff:2 * ff] = w3[0]
    w_all[near, 2 * ff:3 * ff] = w2[0]

    block = 4
    n = block * capacity
    for b in range(0, units, block):
        rows = pl.ds(b * capacity, n)
        x = rows_ref[0, b:b + block, :, 0:d].reshape(n, d)
        dy = rows_ref[0, b:b + block, :, d:2 * d].reshape(n, d)
        meta = meta_ref[0, b:b + block].reshape(n, LANES)
        h = jnp.dot(x, w_all[:, 0:2 * ff], preferred_element_type=F32)
        h1, h3 = h[:, :ff], h[:, ff:]
        sig = jax.nn.sigmoid(h1)
        s = h1 * sig
        a = (s * h3).astype(BF)
        g = (meta[:, 0:1] * dy.astype(F32)).astype(BF)
        da = jnp.dot(g, w_all[:, 2 * ff:3 * ff], preferred_element_type=F32)
        dh3 = (da * s).astype(BF)
        dh1 = (da * h3 * sig * (1.0 + h1 * (1.0 - sig))).astype(BF)
        a_s[rows, :] = a
        g_s[rows, :] = g
        dh_s[rows, 0:ff] = dh1
        dh_s[rows, ff:2 * ff] = dh3
        if b < own:
            dy_w2 = jnp.dot(dy, w_all[:, 2 * ff:3 * ff], preferred_element_type=F32)
            dg = jnp.sum(a.astype(F32) * dy_w2, axis=1, keepdims=True)
            lane = lax.broadcasted_iota(jnp.int32, (n, LANES), 1).astype(F32)
            dg = jnp.where(lane == meta[:, 1:2], dg, 0.0)
            dh = jnp.concatenate([dh1, dh3], axis=1)
            dx = lax.dot_general(dh, w_all[:, 0:2 * ff], NT, preferred_element_type=F32)
            to_x, to_g, at = (dx_mine, dg_mine, b) if b < mine else (dx_peer, dg_peer, b - mine)
            to_x[0, at:at + block] = dx.astype(BF).reshape(block, capacity, d)
            to_g[0, at:at + block] = dg.reshape(block, capacity, LANES)

    window = acc_s.shape[0]
    lo = pl.multiple_of(f * (d - window), LANES)
    keep = pl.ds(pl.multiple_of(f * (window - half), window - half), half)
    x_win = rows_ref[0, :, :, pl.ds(lo, window)].reshape(total, window)
    acc_s[:, 0:2 * ff] = lax.dot_general(x_win, dh_s[...], TN, preferred_element_type=F32)
    acc_s[:, 2 * ff:3 * ff] = lax.dot_general(g_s[:, pl.ds(lo, window)], a_s[...], TN, preferred_element_type=F32)
    dw1[0] = acc_s[keep, 0:ff]
    dw3[0] = acc_s[keep, ff:2 * ff]
    dw2[0] = acc_s[keep, 2 * ff:3 * ff]


def experts_pass(half, rows, meta, weights, w_got, first, grads, own, mine):
    n = w_got.shape[0]
    experts, units, capacity, width = rows.shape
    d = width // 2
    dh, ff = weights[0].shape[1:]
    at = lambda *s: pl.BlockSpec((1,) + s, lambda e: (e + first,) + (0,) * len(s))
    loc = lambda *s: pl.BlockSpec((1,) + s, lambda e: (e,) + (0,) * len(s))
    anywhere = pl.BlockSpec(memory_space=pl.ANY)
    aliased = grads is not None
    total = units * capacity
    window = -(-dh // LANES) * LANES
    grad = jax.ShapeDtypeStruct((experts, dh, ff), F32)
    flops = n * 2 * total * d * ff * 6
    return pl.pallas_call(
        functools.partial(expert_kernel, aliased=aliased, own=own, mine=mine),
        grid=(n,),
        in_specs=[pl.BlockSpec(memory_space=pltpu.SMEM), at(units, capacity, width), at(units, capacity, LANES)]
        + [at(dh, ff)] * 3 + [loc(dh, 3 * ff)] + [anywhere] * (3 if aliased else 0),
        out_specs=[at(dh, ff)] * 3 + [loc(mine, capacity, d), loc(own - mine, capacity, d),
                                      loc(mine, capacity, LANES), loc(own - mine, capacity, LANES)],
        out_shape=[
            grad,
            grad,
            grad,
            jax.ShapeDtypeStruct((n, mine, capacity, d), BF),
            jax.ShapeDtypeStruct((n, own - mine, capacity, d), BF),
            jax.ShapeDtypeStruct((n, mine, capacity, LANES), F32),
            jax.ShapeDtypeStruct((n, own - mine, capacity, LANES), F32),
        ],
        scratch_shapes=[
            pltpu.VMEM((d, 3 * ff), BF),
            pltpu.VMEM((total, d), BF),
            pltpu.VMEM((total, ff), BF),
            pltpu.VMEM((total, 2 * ff), BF),
            pltpu.VMEM((window, 3 * ff), F32),
        ],
        input_output_aliases={7: 0, 8: 1, 9: 2} if aliased else {},
        compiler_params=params(),
        cost_estimate=cost(flops, n * total * width * 2),
        name="experts",
    )(half, rows, meta, *weights, w_got, *(grads if aliased else ()))


def combine_kernel(*refs, top_k, has_prev, last):
    pos_own, pos_peer, dx_own, dx_peer, dg_own, dg_peer = refs[:6]
    prev = refs[6] if has_prev else None
    refs = refs[6 + (1 if has_prev else 0):]
    if last:
        sum_ref, gate_ref, acc, rhs = refs
    else:
        acc, rhs = refs
        acc = acc.at[0]
    group, _, capacity, d = dx_own.shape
    tokens = pos_own.shape[2]
    g = pl.program_id(1)

    @pl.when(g == 0)
    def _():
        if has_prev:
            acc[...] = prev[0]
        else:
            acc[...] = jnp.zeros(acc.shape, F32)

    n = group * capacity
    for i, (dx, dg) in enumerate(((dx_own, dg_own), (dx_peer, dg_peer))):
        rhs[i * n:(i + 1) * n, 0:d] = dx[...].reshape(n, d)
        val = dg[...].reshape(n, LANES)
        high = val.astype(BF).astype(F32)
        mid = (val - high).astype(BF).astype(F32)
        low = val - high - mid
        packed = high + pltpu.roll(mid, top_k, 1) + pltpu.roll(low, 2 * top_k, 1)
        rhs[i * n:(i + 1) * n, d:d + LANES] = packed.astype(BF)
    slot = lax.broadcasted_iota(jnp.int32, (capacity, tokens), 0).astype(F32).astype(BF)
    picks = []
    for pos in (pos_own, pos_peer):
        for e in range(group):
            row = jnp.broadcast_to(pos[0, e:e + 1, :], (capacity, tokens))
            picks.append(jnp.where(row == slot, jnp.ones((), BF), jnp.zeros((), BF)))
    one_hot = jnp.concatenate(picks, axis=0)
    acc[...] += lax.dot_general(one_hot, rhs[...], TN, preferred_element_type=F32)
    if last:
        @pl.when(g == pl.num_programs(1) - 1)
        def _():
            sum_ref[0] = acc[:, 0:d]
            part = acc[:, d:d + LANES]
            part = part + pltpu.roll(part, LANES - top_k, 1) + pltpu.roll(part, LANES - 2 * top_k, 1)
            gate_ref[0] = part.T[0:top_k, :]


def combine(pos_own, pos_peer, pieces, prev, first, unit0, units, top_k, last):
    dx_own, dx_peer, dg_own, dg_peer = pieces
    n, _, capacity, d = dx_own.shape
    tokens = pos_own.shape[2]
    group = 4 if n % GROUP else GROUP
    assert first % group == 0
    base = first // group
    table = pl.BlockSpec((1, group, tokens), lambda u, g: (u + unit0, g + base, 0))
    rows = lambda w: pl.BlockSpec((group, 1, capacity, w), lambda u, g: (g, u + unit0, 0, 0))
    whole = lambda shift, *s: pl.BlockSpec((1,) + s, lambda u, g: (u + shift,) + (0,) * len(s))
    has_prev = prev is not None
    wide = d + LANES
    if last:
        out_specs = [whole(0, tokens, d), whole(0, top_k, tokens)]
        out_shape = [jax.ShapeDtypeStruct((units, tokens, d), F32), jax.ShapeDtypeStruct((units, top_k, tokens), F32)]
        scratch = [pltpu.VMEM((tokens, wide), F32)]
    else:
        out_specs = whole(0, tokens, wide)
        out_shape = jax.ShapeDtypeStruct((units, tokens, wide), F32)
        scratch = []
    scratch = scratch + [pltpu.VMEM((2 * group * capacity, wide), BF)]
    return pl.pallas_call(
        functools.partial(combine_kernel, top_k=top_k, has_prev=has_prev, last=last),
        grid=(units, n // group),
        in_specs=[table, table, rows(d), rows(d), rows(LANES), rows(LANES)]
        + ([pl.BlockSpec((1, tokens, wide), lambda u, g: (u + unit0, 0, 0))] if has_prev else []),
        out_specs=out_specs,
        out_shape=out_shape,
        scratch_shapes=scratch,
        compiler_params=params(),
        cost_estimate=cost(4 * units * n * capacity * tokens * wide, units * tokens * wide * 8),
        name="combine",
    )(pos_own, pos_peer, dx_own, dx_peer, dg_own, dg_peer, *((prev,) if has_prev else ()))


def solution(mesh):
    tok_spec = P(None, ('fsdp', 'ep'), None)
    spec_edf = P('ep', 'fsdp', None)
    spec_efd = P('ep', None, 'fsdp')

    def over_y(v):
        return lax.ppermute(v, 'fsdp', [(0, 1), (1, 0)])

    def over_x(v):
        return lax.ppermute(v, 'ep', [(0, 2), (1, 3), (2, 0), (3, 1)])

    def over_core(v):
        return lax.ppermute(v, 'ep', [(0, 1), (1, 0), (2, 3), (3, 2)])

    def step(x_in, dy_out, expert_idx, gate_prob, w_one, w_two, w_three):
        micro, tokens, _ = x_in.shape
        top_k = expert_idx.shape[2]
        local = w_one.shape[0]
        capacity = capacity_of(tokens, top_k, local * 4)
        f, ep = lax.axis_index('fsdp'), lax.axis_index('ep')
        half = f.astype(jnp.int32).reshape(1)
        base_own = (ep * local).astype(jnp.int32).reshape(1)
        base_peer = ((ep ^ 1) * local).astype(jnp.int32).reshape(1)

        def tables(info, base=base_own):
            return route(base, info, local, top_k, capacity)

        info = jnp.concatenate([jnp.swapaxes(expert_idx, 1, 2).astype(F32), jnp.swapaxes(gate_prob, 1, 2)], axis=1)
        b = [jnp.concatenate([x_in[m], dy_out[m]], axis=1) for m in range(micro)]
        iy = over_y(info)
        ix = over_x(info)
        ic = over_core(info)
        near = jnp.concatenate([iy, ix])
        near_c = over_core(near)
        idg = over_x(iy)
        idc = over_core(idg)
        t_own = tables(info)
        t_core = tables(ic)
        t_near = tables(jnp.concatenate([near, near_c]))
        t_diag = tables(jnp.concatenate([idg, idc]))
        pos_own = jnp.concatenate([t_own[0], t_near[0][2:4]])
        pos_peer = tables(jnp.concatenate([info, ix]), base_peer)[0]

        w_two_t = jnp.swapaxes(w_two, 1, 2)
        weights = (w_one, w_three, w_two_t)
        y = [over_y(b[m]) for m in range(micro)]
        x = [over_x(b[m]) for m in range(micro)]
        d = [over_x(y[m]) for m in range(micro)]
        bc, yc, xc, dc = ([over_core(v[m]) for m in range(micro)] for v in (b, y, x, d))
        got = []
        first = 0
        for n in CHUNKS:
            got.append(over_y(jnp.concatenate([w[first:first + n] for w in weights], axis=2)))
            first += n

        calls = [
            (t_own, (0, 1), b, (0, 1)),
            (t_core, (0, 1), bc, (4, 1)),
            (t_near, (0, 2), [y[0], x[0]], (8, -6)),
            (t_near, (4, 2), [yc[0], xc[0]], (12, -6)),
            (t_near, (1, 2), [y[1], x[1]], (9, -6)),
            (t_near, (5, 2), [yc[1], xc[1]], (13, -6)),
            (t_diag, (0, 2), [d[0], dc[0]], (10, 4)),
            (t_diag, (1, 2), [d[1]], (11, 4)),
            (t_diag, (3, 2), [dc[1]], (15, 4)),
        ]
        buffers = None
        for table, start, blocks, place in calls:
            buffers = gather(table, start, blocks, place, 16, capacity, buffers)
        rows, meta = buffers

        grads = None
        partial = None
        first = 0
        for k, n in enumerate(CHUNKS):
            res = experts_pass(half, rows, meta, weights, got[k], first, grads, 8, 4)
            grads = res[:3]
            pieces = (res[3], over_core(res[4]), res[5], over_core(res[6]))

            def combined(*rest):
                return combine(pos_own, pos_peer, pieces, partial, first, *rest)

            if k + 1 < len(CHUNKS):
                partial = combined(0, 4, top_k, False)
            else:
                away = [combined(2 + m, 1, top_k, True) for m in range(micro)]
                back = [(over_x(away[m][0]), over_x(away[m][1])) for m in range(micro)]
                home = [combined(m, 1, top_k, True) for m in range(micro)]
            first += n
        dx = [(h[0][0] + r[0][0]).astype(BF) for h, r in zip(home, back)]
        dg = [(h[1][0] + r[1][0]).T for h, r in zip(home, back)]
        return jnp.stack(dx), jnp.stack(dg), grads[0], jnp.swapaxes(grads[2], 1, 2), grads[1]

    return jax.shard_map(step, mesh=mesh, in_specs=(tok_spec, tok_spec, tok_spec, tok_spec, spec_edf, spec_efd, spec_edf), out_specs=(tok_spec, tok_spec, spec_edf, spec_efd, spec_edf), check_vma=False)
```
